32 devices in a mesh: dp: 1 (over z), hp: 4 (over y), sp: 8 (over x, core).
Axes of the slice: x: 4, y: 4, z: 1, core: 2. Of those that a mesh axis runs over, the one named last changes fastest.
The devices are a block of a 4x4x8 slice.
Arguments:
- x_in: bfloat16 [4096, 8192], P(('dp', 'sp', 'hp'))
- w_q: bfloat16 [8192, 8192], P(None, 'hp')
- w_k: bfloat16 [8192, 8192], P(None, 'hp')
- w_v: bfloat16 [8192, 8192], P(None, 'hp')
- w_o: bfloat16 [8192, 8192], P('hp')
Outputs:
- output: bfloat16 [4096, 8192], P(('dp', 'sp', 'hp'))
All inputs are finite; a program needn't handle non-finite values.
Results may differ from the reference program's by a relative error of at most 0.007578.
Values are sent between devices in bfloat16 or wider.
A program may use at most 768 MiB of HBM per device.

```python
import math
import jax
import jax.numpy as jnp
from jax import lax

D = 8192
H = 64
HKV = 64
HEAD = 128
SEQ = 4096
QBLK = 64
GROUP = H // HKV


def setup_inputs(seed: int = 0, part: int = 0) -> dict:
    root = jax.random.key(seed)
    shared_key, part_root = jax.random.split(root)
    part_key = jax.random.fold_in(part_root, part)
    key_q, key_k, key_v, key_o = jax.random.split(shared_key, 4)
    logit_std = math.sqrt(max(math.log(SEQ / 16.0), 1.0))
    qk_gain = math.sqrt(logit_std) / math.sqrt(D)
    x_in = jax.random.normal(part_key, (SEQ, D), jnp.float32).astype(jnp.bfloat16)
    w_q = (jax.random.normal(key_q, (D, H * HEAD), jnp.float32) * qk_gain).astype(jnp.bfloat16)
    w_k = (jax.random.normal(key_k, (D, HKV * HEAD), jnp.float32) * qk_gain).astype(jnp.bfloat16)
    w_v = (jax.random.normal(key_v, (D, HKV * HEAD), jnp.float32) / math.sqrt(D)).astype(jnp.bfloat16)
    w_o = (jax.random.normal(key_o, (H * HEAD, D), jnp.float32) * (4.0 / math.sqrt(H * HEAD))).astype(jnp.bfloat16)
    return {'x_in': x_in, 'w_q': w_q, 'w_k': w_k, 'w_v': w_v, 'w_o': w_o}


def reference(x_in, w_q, w_k, w_v, w_o):
    q_all = jnp.dot(x_in, w_q, preferred_element_type=jnp.float32).astype(jnp.bfloat16)
    k_all = jnp.dot(x_in, w_k, preferred_element_type=jnp.float32).astype(jnp.bfloat16)
    v_all = jnp.dot(x_in, w_v, preferred_element_type=jnp.float32).astype(jnp.bfloat16)
    q_heads = q_all.astype(jnp.float32).reshape(SEQ, HKV, GROUP, HEAD)
    k_heads = k_all.astype(jnp.float32).reshape(SEQ, HKV, HEAD)
    v_heads = v_all.astype(jnp.float32).reshape(SEQ, HKV, HEAD)
    attn_scale = 1.0 / math.sqrt(HEAD)

    def query_block(blk_index):
        q_blk = lax.dynamic_slice_in_dim(q_heads, blk_index * QBLK, QBLK, 0)
        scores = jnp.einsum('qhgd,khd->hgqk', q_blk, k_heads) * attn_scale
        row_max = jnp.max(scores, axis=-1, keepdims=True)
        prob_vals = jnp.exp(scores - row_max)
        row_sum = jnp.sum(prob_vals, axis=-1, keepdims=True)
        weighted = jnp.einsum('hgqk,khd->hgqd', prob_vals.astype(jnp.bfloat16).astype(jnp.float32), v_heads)
        out_blk = (weighted / row_sum).astype(jnp.bfloat16)
        return jnp.transpose(out_blk, (2, 0, 1, 3)).reshape(QBLK, H * HEAD)

    o_all = lax.map(query_block, jnp.arange(SEQ // QBLK)).reshape(SEQ, H * HEAD)
    return jnp.dot(o_all, w_o, preferred_element_type=jnp.float32).astype(jnp.bfloat16)
```

```python
import functools
import math

import jax
import jax.numpy as jnp
from jax import lax
from jax.experimental import pallas as pl
from jax.experimental.pallas import tpu as pltpu
from jax.sharding import PartitionSpec as P

HEAD_DIM = 128
CORES = 2
RING = 4
MESH_ID = pl.DeviceIdType.MESH
VMEM_BYTES = 64_000_000


def remote(src, dst, send_sem, recv_sem, sp, hp):
    return pltpu.make_async_remote_copy(
        src_ref=src, dst_ref=dst, send_sem=send_sem, recv_sem=recv_sem,
        device_id={'sp': sp, 'hp': hp}, device_id_type=MESH_ID)


def entry_barrier(peers):
    barrier = pltpu.get_barrier_semaphore()
    for sp, hp in peers:
        pl.semaphore_signal(barrier, inc=1, device_id={'sp': sp, 'hp': hp}, device_id_type=MESH_ID)
    pl.semaphore_wait(barrier, len(peers))


def qkv_kernel(x_ref, wq_ref, wk_ref, wv_ref, out_ref, xbuf, wbuf, obuf,
               own_send, relay_send, pair_send, load_sem, x_recv, w_sem, out_send, out_recv, out_local):
    sp, hp = lax.axis_index('sp'), lax.axis_index('hp')
    core, chip = lax.rem(sp, CORES), sp // CORES
    partner = sp + 1 - 2 * core
    up, down = lax.rem(hp + 1, RING), lax.rem(hp + RING - 1, RING)
    rows = x_ref.shape[0]
    half = rows // 2
    width = wbuf.shape[2] // 2
    mine, other = core * rows, (1 - core) * rows
    chips = [lax.rem(chip + d, RING) for d in range(RING)]
    ranks = [c * CORES + core for c in chips]

    def slot(p, base, side):
        return xbuf.at[p, pl.ds(pl.multiple_of(base + side * half, half), half)]

    def weight_copies(step, start):
        within = lax.rem(step, 6)
        buf = lax.rem(step, 3)
        for m, w_ref in enumerate((wq_ref, wk_ref, wv_ref)):
            for pair, dests in enumerate(((1, 3), (2, 0))):
                @pl.when(within == 2 * m + pair)
                def _():
                    for n, d in enumerate(dests):
                        cols = pl.ds(pl.multiple_of(ranks[d] * width, width), width)
                        copy = pltpu.make_async_copy(
                            w_ref.at[:, cols], wbuf.at[buf, :, pl.ds(n * width, width)], w_sem.at[buf, n])
                        copy.start() if start else copy.wait()

    weight_copies(0, True)
    weight_copies(1, True)
    own_load = pltpu.make_async_copy(x_ref, xbuf.at[0, pl.ds(pl.multiple_of(mine, rows), rows)], load_sem)
    own_load.start()

    entry_barrier([(partner, hp), (sp, up), (sp, down)] + [(ranks[d], hp) for d in (1, 2, 3)])

    first, second = x_ref.at[pl.ds(0, half)], x_ref.at[pl.ds(half, half)]
    own_copies = [
        remote(x_ref, xbuf.at[0, pl.ds(pl.multiple_of(mine, rows), rows)], own_send.at[0], x_recv.at[0, 1, 0], partner, hp),
        remote(first, slot(1, mine, 0), own_send.at[1], x_recv.at[1, 0, 0], sp, up),
        remote(second, slot(1, mine, 1), own_send.at[2], x_recv.at[1, 0, 1], sp, down),
        remote(second, slot(2, mine, 0), own_send.at[3], x_recv.at[2, 0, 0], sp, up),
        remote(first, slot(2, mine, 1), own_send.at[4], x_recv.at[2, 0, 1], sp, down),
    ]
    for copy in own_copies:
        copy.start()

    def from_side(p, side):
        return remote(slot(p, mine, side), slot(p, mine, side), own_send.at[0], x_recv.at[p, 0, side], sp, hp)

    def from_partner(p, side):
        return remote(slot(p, other, side), slot(p, other, side), own_send.at[0], x_recv.at[p, 1, side], sp, hp)

    def to_partner(p, side):
        return remote(slot(p, mine, side), slot(p, mine, side), pair_send.at[p - 1, side], x_recv.at[p, 1, side],
                      partner, hp)

    def relays():
        return [remote(slot(1, mine, 0), slot(3, mine, 0), relay_send.at[0], x_recv.at[3, 0, 0], sp, up),
                remote(slot(1, mine, 1), slot(3, mine, 1), relay_send.at[1], x_recv.at[3, 0, 1], sp, down)]

    def begin_pass(p):
        if p == 0:
            own_load.wait()
            whole = xbuf.at[0, pl.ds(pl.multiple_of(other, rows), rows)]
            remote(whole, whole, own_send.at[0], x_recv.at[0, 1, 0], sp, hp).wait_recv()
            return
        for side in (0, 1):
            from_side(p, side).wait_recv()
            if p == 1:
                relays()[side].start()
            to_partner(p, side).start()
        for side in (0, 1):
            from_partner(p, side).wait_recv()

    def send_out(step):
        p, within = step // 6, lax.rem(step, 6)
        for m in range(3):
            for pair, dests in enumerate(((1, 3), (2, 0))):
                @pl.when(within == 2 * m + pair)
                def _():
                    for n, d in enumerate(dests):
                        src, dst = obuf.at[step, n], out_ref.at[m, chip, p]
                        if d == 0:
                            pltpu.make_async_copy(src, dst, out_local).start()
                        else:
                            remote(src, dst, out_send, out_recv, ranks[d], hp).start()

    steps = 6 * RING

    def body(step, carry):
        for p in range(RING):
            @pl.when(step == 6 * p)
            def _():
                begin_pass(p)

        @pl.when(step + 2 < steps)
        def _():
            weight_copies(step + 2, True)

        weight_copies(step, False)
        buf = lax.rem(step, 3)
        prod = jnp.dot(xbuf[step // 6], wbuf[buf], preferred_element_type=jnp.float32).astype(jnp.bfloat16)
        obuf[step, 0] = prod[:, :width]
        obuf[step, 1] = prod[:, width:]

        @pl.when(step > 0)
        def _():
            send_out(step - 1)
        return carry

    lax.fori_loop(0, steps, body, 0)
    for copy in own_copies:
        copy.wait_send()
    for copy in relays():
        copy.wait_send()
    for p in (1, 2, 3):
        for side in (0, 1):
            to_partner(p, side).wait_send()
    send_out(jnp.int32(steps - 1))
    local_part, remote_part = obuf.at[pl.ds(0, 6)], obuf.at[pl.ds(0, 18)]
    pltpu.make_async_copy(local_part, local_part, out_local).wait()
    remote(remote_part, remote_part, out_send, out_recv, sp, hp).wait()


def attend_kernel(qkv_ref, o_ref, q_vm, k_vm, v_vm, vt_vm, s_even, s_odd, m_even, m_odd, o_vm,
                  load_sem, o_send, o_recv, o_local):
    sp, hp = lax.axis_index('sp'), lax.axis_index('hp')
    core, chip = lax.rem(sp, CORES), sp // CORES
    partner = sp + 1 - 2 * core
    blocks, block = q_vm.shape[0], q_vm.shape[1]
    rows, half = block // 2, block // 4
    scale = HEAD_DIM ** -0.5 * math.log2(math.e)
    strip = min(block, 32)

    loads = [pltpu.make_async_copy(qkv_ref.at[m], dst, load_sem.at[m]) for m, dst in enumerate((q_vm, k_vm, v_vm))]
    for copy in loads:
        copy.start()
    others = [(d, k) for d in range(RING) for k in range(CORES) if (d, k) != (0, 0)]
    rank_of = lambda d, k: lax.rem(chip + d, RING) * CORES + lax.rem(core + k, CORES)
    entry_barrier([(rank_of(d, k), hp) for d, k in others])
    for copy in loads:
        copy.wait()

    def turn(b, carry):
        vt_vm[b] = v_vm[b].astype(jnp.float32).T.astype(jnp.bfloat16)
        return carry

    lax.fori_loop(0, blocks, turn, 0)

    def which(i):
        return lax.rem(chip + 1 + lax.rem(i, RING), RING) * RING + lax.rem(i // RING + 1, RING)

    def lanes(head):
        return slice(head * HEAD_DIM, (head + 1) * HEAD_DIM)

    def scores(q_blk, head, chunk):
        return lax.dot_general(k_vm[chunk, :, lanes(head)], q_blk, (((1,), (1,)), ((), ())),
                               preferred_element_type=jnp.float32)

    def fold(x, op):
        parts = x.reshape(block // strip, strip, block)
        return op(parts, axis=0)

    def stage(q_next, next_head, s_next, m_next, s_now, m_now, head):
        shift = None if s_now is None else jnp.max(m_now[...], axis=0, keepdims=True) * scale
        peak = total = acc = None
        for chunk in range(blocks):
            s = scores(q_next, next_head, chunk)
            s_next[chunk] = s
            top = fold(s, jnp.max)
            peak = top if peak is None else jnp.maximum(peak, top)
            if s_now is not None:
                prob = jnp.exp2(s_now[chunk] * scale - shift)
                part = fold(prob, jnp.sum)
                total = part if total is None else total + part
                pv = jnp.dot(vt_vm[chunk, lanes(head), :], prob.astype(jnp.bfloat16), preferred_element_type=jnp.float32)
                acc = pv if acc is None else acc + pv
        m_next[...] = peak
        if s_now is None:
            return None
        return (acc / jnp.sum(total, axis=0, keepdims=True)).T.astype(jnp.bfloat16)

    stage(q_vm[which(0), :, lanes(0)], 0, s_even, m_even, None, None, 0)

    def send_home(i):
        d, p = lax.rem(i + 1, RING), lax.rem(i // RING + 1, RING)
        home = lax.rem(chip + d, RING) * CORES
        for pp in range(RING):
            @pl.when(p == pp)
            def _():
                for k in range(CORES):
                    kk = lax.rem(core + k, CORES)
                    for side in (0, 1):
                        target = (0, 1 + side, 1 + side, 3)[pp]
                        first = (1 - side if pp == 2 else side) * half
                        src = o_vm.at[i, pl.ds(pl.multiple_of(kk * rows + side * half, half), half)]
                        dst = o_ref.at[sp, target, pl.ds(first, half)]
                        if k:
                            remote(src, dst, o_send, o_recv, home + kk, hp).start()
                        else:
                            @pl.when(d == 0)
                            def _():
                                pltpu.make_async_copy(src, dst, o_local).start()

                            @pl.when(d != 0)
                            def _():
                                remote(src, dst, o_send, o_recv, home + kk, hp).start()

    def body(i, carry):
        now, later = which(i), which(lax.rem(i + 1, blocks))
        o_vm[i, :, lanes(0)] = stage(q_vm[now, :, lanes(1)], 1, s_odd, m_odd, s_even, m_even, 0)

        @pl.when(i > 0)
        def _():
            send_home(i - 1)
        o_vm[i, :, lanes(1)] = stage(q_vm[later, :, lanes(0)], 0, s_even, m_even, s_odd, m_odd, 1)
        return carry

    lax.fori_loop(0, blocks, body, 0)
    send_home(jnp.int32(blocks - 1))
    local_part = o_vm.at[pl.ds(0, 2)]
    pltpu.make_async_copy(local_part, local_part, o_local).wait()
    remote_part = o_vm.at[pl.ds(0, 14)]
    remote(remote_part, remote_part, o_send, o_recv, sp, hp).wait()


def project_kernel(o_ref, w_ref, y_ref, o_vm, wbuf, part, recv, load_sem, w_sem, send_sem, recv_sem):
    sp, hp = lax.axis_index('sp'), lax.axis_index('hp')
    ring = (lax.rem(hp + 1, RING), lax.rem(hp + RING - 1, RING))
    tiles, cols = part.shape[0], part.shape[3]
    ranks, _, rows, width = o_vm.shape

    def w_copy(tile):
        buf = lax.rem(tile, 3)
        return pltpu.make_async_copy(w_ref.at[:, pl.ds(pl.multiple_of(tile * cols, cols), cols)], wbuf.at[buf],
                                     w_sem.at[buf])

    load = pltpu.make_async_copy(o_ref, o_vm, load_sem)
    load.start()
    w_copy(0).start()
    w_copy(1).start()
    entry_barrier([(sp, ring[0]), (sp, ring[1])])
    load.wait()
    order = ((1, 3, 2), (2, 3, 1))

    def hop(tile, way, step):
        return remote(part.at[tile, order[way][step]], recv.at[tile, step], send_sem.at[tile, step],
                      recv_sem.at[tile, step], sp, ring[way])

    def compute(pair, carry):
        for way in (0, 1):
            tile = 2 * pair + way

            @pl.when(tile + 2 < tiles)
            def _():
                w_copy(tile + 2).start()
            w_copy(tile).wait()
            buf = lax.rem(tile, 3)
            acc = None
            for r in range(ranks):
                prod = jnp.dot(o_vm[r].reshape(RING * rows, width), wbuf[buf, pl.ds(r * width, width), :],
                               preferred_element_type=jnp.float32)
                acc = prod if acc is None else acc + prod
            part[tile] = acc.reshape(RING, rows, cols)

            @pl.when(tile > 0)
            def _():
                hop(tile - 1, 1 - way, 0).start()
        return carry

    lax.fori_loop(0, tiles // 2, compute, 0)
    hop(jnp.int32(tiles - 1), 1, 0).start()

    for step in (1, 2):
        def pass_on(pair, carry):
            for way in (0, 1):
                tile = 2 * pair + way
                hop(tile, way, step - 1).wait_recv()
                slot = order[way][step]
                part[tile, slot] = part[tile, slot] + recv[tile, step - 1]
            for way in (0, 1):
                hop(2 * pair + way, way, step).start()
            return carry

        lax.fori_loop(0, tiles // 2, pass_on, 0)

    def finish(pair, carry):
        for way in (0, 1):
            tile = 2 * pair + way
            hop(tile, way, 2).wait_recv()
            y_ref[:, pl.ds(pl.multiple_of(tile * cols, cols), cols)] = (part[tile, 0] + recv[tile, 2]).astype(y_ref.dtype)
        return carry

    lax.fori_loop(0, tiles // 2, finish, 0)

    def drain(pair, carry):
        for way in (0, 1):
            for step in range(3):
                hop(2 * pair + way, way, step).wait_send()
        return carry

    lax.fori_loop(0, tiles // 2, drain, 0)


def solution(mesh):
    assert mesh.shape['hp'] == RING and mesh.shape['sp'] == RING * CORES
    ranks = mesh.shape['sp']
    anywhere = pl.BlockSpec(memory_space=pl.ANY)
    dma = pltpu.SemaphoreType.DMA

    def params(ident):
        return pltpu.CompilerParams(collective_id=ident, has_side_effects=True, vmem_limit_bytes=VMEM_BYTES)

    def device_fn(x_loc, w_q, w_k, w_v, w_o):
        rows, depth = x_loc.shape
        width = w_q.shape[1] // ranks
        block = CORES * rows
        blocks = RING * RING
        bf16, f32 = jnp.bfloat16, jnp.float32
        tiles = 16
        cols = w_o.shape[1] // tiles

        qkv = pl.pallas_call(
            qkv_kernel,
            out_shape=jax.ShapeDtypeStruct((3, RING, RING, block, width), bf16),
            in_specs=[anywhere] * 4,
            out_specs=anywhere,
            scratch_shapes=[
                pltpu.VMEM((RING, block, depth), bf16),
                pltpu.VMEM((3, depth, 2 * width), bf16),
                pltpu.VMEM((6 * RING, 2, block, width), bf16),
                dma((5,)), dma((2,)), dma((3, 2)), dma, dma((RING, 2, 2)), dma((3, 2)), dma, dma, dma,
            ],
            compiler_params=params(0),
            name='gather_qkv',
        )(x_loc, w_q, w_k, w_v)

        heads_out = pl.pallas_call(
            attend_kernel,
            out_shape=jax.ShapeDtypeStruct((ranks, RING, rows, width), bf16),
            in_specs=[anywhere],
            out_specs=anywhere,
            scratch_shapes=[
                pltpu.VMEM((blocks, block, width), bf16),
                pltpu.VMEM((blocks, block, width), bf16),
                pltpu.VMEM((blocks, block, width), bf16),
                pltpu.VMEM((blocks, width, block), bf16),
                pltpu.VMEM((blocks, block, block), f32),
                pltpu.VMEM((blocks, block, block), f32),
                pltpu.VMEM((min(block, 32), block), f32),
                pltpu.VMEM((min(block, 32), block), f32),
                pltpu.VMEM((blocks, block, width), bf16),
                dma((3,)), dma, dma, dma,
            ],
            compiler_params=params(1),
            name='attend',
        )(qkv.reshape(3, blocks, block, width))

        return pl.pallas_call(
            project_kernel,
            out_shape=jax.ShapeDtypeStruct((rows, w_o.shape[1]), bf16),
            in_specs=[anywhere] * 2,
            out_specs=pl.BlockSpec(memory_space=pltpu.VMEM),
            scratch_shapes=[
                pltpu.VMEM((ranks, RING, rows, width), bf16),
                pltpu.VMEM((3, w_o.shape[0], cols), bf16),
                pltpu.VMEM((tiles, RING, rows, cols), f32),
                pltpu.VMEM((tiles, 3, rows, cols), f32),
                dma, dma((3,)), dma((tiles, 3)), dma((tiles, 3)),
            ],
            compiler_params=params(2),
            name='project',
        )(heads_out, w_o)

    seq_spec = P(('dp', 'sp', 'hp'), None)
    in_specs = (seq_spec, P(None, 'hp'), P(None, 'hp'), P(None, 'hp'), P('hp', None))
    return jax.shard_map(device_fn, mesh=mesh, in_specs=in_specs, out_specs=seq_spec, check_vma=False)
```

```python
import functools
import math

import jax
import jax.numpy as jnp
from jax import lax
from jax.experimental import pallas as pl
from jax.experimental.pallas import tpu as pltpu
from jax.sharding import PartitionSpec as P

HEAD_DIM = 128
CORES = 2
RING = 4
PAIRS = ((2, 0), (1, 3))
MESH_ID = pl.DeviceIdType.MESH
VMEM_BYTES = 66_000_000


def remote(src, dst, send_sem, recv_sem, sp, hp):
    return pltpu.make_async_remote_copy(
        src_ref=src, dst_ref=dst, send_sem=send_sem, recv_sem=recv_sem,
        device_id={'sp': sp, 'hp': hp}, device_id_type=MESH_ID)


def entry_barrier(peers):
    barrier = pltpu.get_barrier_semaphore()
    for sp, hp in peers:
        pl.semaphore_signal(barrier, inc=1, device_id={'sp': sp, 'hp': hp}, device_id_type=MESH_ID)
    pl.semaphore_wait(barrier, len(peers))


def qkv_kernel(x_ref, wq_ref, wk_ref, wv_ref, out_ref, xbuf, wbuf, obuf, via,
               own_send, relay_send, pair_send, load_sem, x_recv, w_sem, out_send, out_recv, out_local, via_recv, via_send):
    sp, hp = lax.axis_index('sp'), lax.axis_index('hp')
    core, chip = lax.rem(sp, CORES), sp // CORES
    partner = sp + 1 - 2 * core
    up, down = lax.rem(hp + 1, RING), lax.rem(hp + RING - 1, RING)
    rows = x_ref.shape[0]
    half = rows // 2
    width = wbuf.shape[2] // 2
    mine, other = core * rows, (1 - core) * rows
    chips = [lax.rem(chip + d, RING) for d in range(RING)]
    ranks = [c * CORES + core for c in chips]

    def slot(p, base, side):
        return xbuf.at[p, pl.ds(pl.multiple_of(base + side * half, half), half)]

    def weight_copies(step, start):
        within = lax.rem(step, 6)
        buf = lax.rem(step, 3)
        for m, w_ref in enumerate((wq_ref, wk_ref, wv_ref)):
            for pair, dests in enumerate(PAIRS):
                @pl.when(within == 3 * pair + m)
                def _():
                    for n, d in enumerate(dests):
                        cols = pl.ds(pl.multiple_of(ranks[d] * width, width), width)
                        copy = pltpu.make_async_copy(
                            w_ref.at[:, cols], wbuf.at[buf, :, pl.ds(n * width, width)], w_sem.at[buf, n])
                        copy.start() if start else copy.wait()

    weight_copies(0, True)
    weight_copies(1, True)
    own_load = pltpu.make_async_copy(x_ref, xbuf.at[0, pl.ds(pl.multiple_of(mine, rows), rows)], load_sem)
    own_load.start()

    entry_barrier([(partner, hp), (sp, up), (sp, down)] + [(ranks[d], hp) for d in (1, 2, 3)])

    first, second = x_ref.at[pl.ds(0, half)], x_ref.at[pl.ds(half, half)]
    own_copies = [
        remote(x_ref, xbuf.at[0, pl.ds(pl.multiple_of(mine, rows), rows)], own_send.at[0], x_recv.at[0, 1, 0], partner, hp),
        remote(first, slot(1, mine, 0), own_send.at[1], x_recv.at[1, 0, 0], sp, up),
        remote(second, slot(1, mine, 1), own_send.at[2], x_recv.at[1, 0, 1], sp, down),
        remote(second, slot(2, mine, 0), own_send.at[3], x_recv.at[2, 0, 0], sp, up),
        remote(first, slot(2, mine, 1), own_send.at[4], x_recv.at[2, 0, 1], sp, down),
    ]
    for copy in own_copies:
        copy.start()

    def from_side(p, side):
        return remote(slot(p, mine, side), slot(p, mine, side), own_send.at[0], x_recv.at[p, 0, side], sp, hp)

    def from_partner(p, side):
        return remote(slot(p, other, side), slot(p, other, side), own_send.at[0], x_recv.at[p, 1, side], sp, hp)

    def to_partner(p, side):
        return remote(slot(p, mine, side), slot(p, mine, side), pair_send.at[p - 1, side], x_recv.at[p, 1, side],
                      partner, hp)

    def relays():
        return [remote(slot(1, mine, 0), slot(3, mine, 0), relay_send.at[0], x_recv.at[3, 0, 0], sp, up),
                remote(slot(1, mine, 1), slot(3, mine, 1), relay_send.at[1], x_recv.at[3, 0, 1], sp, down)]

    def begin_pass(p):
        if p == 0:
            own_load.wait()
            whole = xbuf.at[0, pl.ds(pl.multiple_of(other, rows), rows)]
            remote(whole, whole, own_send.at[0], x_recv.at[0, 1, 0], sp, hp).wait_recv()
            return
        for side in (0, 1):
            from_side(p, side).wait_recv()
            if p == 1:
                relays()[side].start()
            to_partner(p, side).start()
        for side in (0, 1):
            from_partner(p, side).wait_recv()

    def send_out(step):
        p, within = step // 6, lax.rem(step, 6)
        for m in range(3):
            for pair, dests in enumerate(PAIRS):
                @pl.when(within == 3 * pair + m)
                def _():
                    for n, d in enumerate(dests):
                        src, dst = obuf.at[step, n], out_ref.at[m, chip, p]
                        if d == 0:
                            pltpu.make_async_copy(src, dst, out_local).start()
                        elif d == 2:
                            for way in (0, 1):
                                remote(src.at[pl.ds(way * rows, rows)], via.at[way, 3 * p + m], out_send,
                                       via_recv.at[way, 3 * p + m], ranks[1 + 2 * way], hp).start()
                        else:
                            remote(src, dst, out_send, out_recv, ranks[d], hp).start()

    def forward(p, m):
        for way in (0, 1):
            spot = via.at[way, 3 * p + m]
            remote(spot, spot, via_send, via_recv.at[way, 3 * p + m], sp, hp).wait_recv()
            remote(spot, out_ref.at[m, chips[3 - 2 * way], p, pl.ds(way * rows, rows)], via_send, out_recv,
                   ranks[1 + 2 * way], hp).start()

    steps = 6 * RING

    def body(step, carry):
        @pl.when(step + 2 < steps)
        def _():
            weight_copies(step + 2, True)

        for m in range(3):
            @pl.when((lax.rem(step + 2, 6) == m) & (step >= 4))
            def _():
                forward((step - 4) // 6, m)

        for p in range(RING):
            @pl.when(step == 6 * p)
            def _():
                begin_pass(p)

        weight_copies(step, False)
        buf = lax.rem(step, 3)
        prod = jnp.dot(xbuf[step // 6], wbuf[buf], preferred_element_type=jnp.float32).astype(jnp.bfloat16)
        obuf[step, 0] = prod[:, :width]
        obuf[step, 1] = prod[:, width:]

        @pl.when(step > 0)
        def _():
            send_out(step - 1)
        return carry

    lax.fori_loop(0, steps, body, 0)
    for copy in own_copies:
        copy.wait_send()
    for copy in relays():
        copy.wait_send()
    for p in (1, 2, 3):
        for side in (0, 1):
            to_partner(p, side).wait_send()
    send_out(jnp.int32(steps - 1))
    forward(RING - 1, 2)
    local_part, remote_part = obuf.at[pl.ds(0, 6)], obuf.at[pl.ds(0, 18)]
    pltpu.make_async_copy(local_part, local_part, out_local).wait()
    remote(remote_part, remote_part, out_send, out_recv, sp, hp).wait()
    remote(via, via, via_send, out_recv, sp, hp).wait_send()


def attend_project_kernel(qkv_ref, w_ref, y_ref, q_vm, k_vm, vt_vm, s_even, s_odd, m_even, m_odd, o_vm, o_rx, wbuf, part,
                          recv, load_sem, o_send, o_recv, w_sem, send_sem, recv_sem):
    sp, hp = lax.axis_index('sp'), lax.axis_index('hp')
    core, chip = lax.rem(sp, CORES), sp // CORES
    ring = (lax.rem(hp + 1, RING), lax.rem(hp + RING - 1, RING))
    blocks, block = q_vm.shape[0], q_vm.shape[1]
    rows, half = block // 2, block // 4
    ranks, width = o_rx.shape[1], o_rx.shape[3]
    tiles, cols = part.shape[0], part.shape[3]
    group = tiles // RING
    depth = wbuf.shape[0]
    scale = HEAD_DIM ** -0.5 * math.log2(math.e)
    strip = min(block, 32)

    loads = [pltpu.make_async_copy(qkv_ref.at[m], dst, load_sem.at[m]) for m, dst in enumerate((q_vm, k_vm, o_vm))]
    for copy in loads:
        copy.start()

    def w_copy(n):
        tile, buf = lax.rem(n, tiles), lax.rem(n, depth)
        return pltpu.make_async_copy(w_ref.at[:, pl.ds(pl.multiple_of(tile * cols, cols), cols)], wbuf.at[buf],
                                     w_sem.at[buf])

    for n in range(depth - 1):
        w_copy(jnp.int32(n)).start()
    others = [(d, k) for d in range(RING) for k in range(CORES) if (d, k) != (0, 0)]
    rank_of = lambda d, k: lax.rem(chip + d, RING) * CORES + lax.rem(core + k, CORES)
    entry_barrier([(rank_of(d, k), hp) for d, k in others] + [(sp, ring[0]), (sp, ring[1])])
    for copy in loads:
        copy.wait()

    def turn(b, carry):
        vt_vm[b] = o_vm[b].astype(jnp.float32).T.astype(jnp.bfloat16)
        return carry

    lax.fori_loop(0, blocks, turn, 0)

    def which(i):
        return lax.rem(chip + 1 + lax.rem(i, RING), RING) * RING + lax.rem(i // RING + 1, RING)

    def lanes(head):
        return slice(head * HEAD_DIM, (head + 1) * HEAD_DIM)

    def scores(q_blk, head, chunk):
        return lax.dot_general(k_vm[chunk, :, lanes(head)], q_blk, (((1,), (1,)), ((), ())),
                               preferred_element_type=jnp.float32)

    def fold(x, op):
        parts = x.reshape(block // strip, strip, block)
        return op(parts, axis=0)

    def stage(q_next, next_head, s_next, m_next, s_now, m_now, head):
        shift = None if s_now is None else jnp.max(m_now[...], axis=0, keepdims=True) * scale
        peak = total = acc = None
        for chunk in range(blocks):
            s = scores(q_next, next_head, chunk)
            s_next[chunk] = s
            top = fold(s, jnp.max)
            peak = top if peak is None else jnp.maximum(peak, top)
            if s_now is not None:
                prob = jnp.exp2(s_now[chunk] * scale - shift)
                add = fold(prob, jnp.sum)
                total = add if total is None else total + add
                pv = jnp.dot(vt_vm[chunk, lanes(head), :], prob.astype(jnp.bfloat16), preferred_element_type=jnp.float32)
                acc = pv if acc is None else acc + pv
        m_next[...] = peak
        if s_now is None:
            return None
        return (acc / jnp.sum(total, axis=0, keepdims=True)).T.astype(jnp.bfloat16)

    stage(q_vm[which(0), :, lanes(0)], 0, s_even, m_even, None, None, 0)

    def send_home(i):
        d, turn_no = lax.rem(i + 1, RING), i // RING
        home = lax.rem(chip + d, RING) * CORES
        for k in range(CORES):
            kk = lax.rem(core + k, CORES)
            piece = pl.ds(pl.multiple_of(kk * rows, rows), rows)

            def away():
                remote(o_vm.at[i, piece], o_rx.at[turn_no, sp], o_send, o_recv.at[turn_no], home + kk, hp).start()

            if k:
                away()
            else:
                pl.when(d != 0)(away)

                @pl.when(d == 0)
                def _():
                    o_rx[turn_no, sp] = o_vm[i, piece]

    order = ((1, 3, 2), (2, 3, 1))

    def hop(tile, way, step):
        return remote(part.at[tile, order[way][step]], recv.at[tile, step], send_sem.at[tile, step],
                      recv_sem.at[tile, step], sp, ring[way])

    def spot(turn_no, side):
        late, second = turn_no // 2, lax.rem(turn_no, 2)
        slot = (1 - late) * (1 + side) + late * (3 - 3 * second)
        first = (1 - late) * second * (1 - 2 * side) + side
        return slot, pl.ds(pl.multiple_of(first * half, half), half)

    def ship(n, way):
        turn_no, tile = n // tiles, lax.rem(n, tiles)

        @pl.when(turn_no < 2)
        def _():
            _, piece = spot(turn_no, way)
            remote(part.at[tile, order[way][0], piece], recv.at[tile, 0, piece], send_sem.at[tile, 0],
                   recv_sem.at[tile, 0], sp, ring[way]).start()

        @pl.when(turn_no == 2)
        def _():
            hop(tile, way, 1).start()

    def project(g):
        turn_no = g // RING

        @pl.when(lax.rem(g, RING) == 0)
        def _():
            seven = o_rx.at[turn_no, pl.ds(0, ranks - 1)]
            remote(seven, seven, o_send, o_recv.at[turn_no], sp, hp).wait_recv()

        for j in range(group):
            n, way = g * group + j, j % 2
            tile, buf = lax.rem(n, tiles), lax.rem(n, depth)

            @pl.when(n + depth - 1 < RING * tiles)
            def _():
                w_copy(n + depth - 1).start()
            w_copy(n).wait()
            acc = None
            for r in range(ranks):
                prod = jnp.dot(o_rx[turn_no, r], wbuf[buf, pl.ds(r * width, width), :],
                               preferred_element_type=jnp.float32)
                acc = prod if acc is None else acc + prod
            for side in (0, 1):
                slot, piece = spot(turn_no, side)
                part[tile, slot, piece] = acc[side * half:(side + 1) * half]

            @pl.when(turn_no == 2)
            def _():
                hop(tile, way, 0).wait_recv()
                part[tile, 3] = part[tile, 3] + recv[tile, 0]

            @pl.when(n > 0)
            def _():
                ship(n - 1, 1 - way)

    def body(i, carry):
        @pl.when(i > 0)
        def _():
            send_home(i - 1)
        now, later = which(i), which(lax.rem(i + 1, blocks))
        o_vm[i, :, lanes(0)] = stage(q_vm[now, :, lanes(1)], 1, s_odd, m_odd, s_even, m_even, 0)
        o_vm[i, :, lanes(1)] = stage(q_vm[later, :, lanes(0)], 0, s_even, m_even, s_odd, m_odd, 1)

        @pl.when(i >= RING)
        def _():
            project(i - RING)
        return carry

    lax.fori_loop(0, blocks, body, 0)
    send_home(jnp.int32(blocks - 1))

    def last_round(g, carry):
        project(g)
        return carry

    lax.fori_loop(blocks - RING, blocks, last_round, 0)

    def pass_on(pair, carry):
        for way in (0, 1):
            tile = 2 * pair + way
            hop(tile, way, 1).wait_recv()
            slot = order[way][2]
            part[tile, slot] = part[tile, slot] + recv[tile, 1]
        for way in (0, 1):
            hop(2 * pair + way, way, 2).start()
        return carry

    lax.fori_loop(0, tiles // 2, pass_on, 0)

    def finish(pair, carry):
        for way in (0, 1):
            tile = 2 * pair + way
            hop(tile, way, 2).wait_recv()
            y_ref[:, pl.ds(pl.multiple_of(tile * cols, cols), cols)] = (part[tile, 0] + recv[tile, 2]).astype(y_ref.dtype)
        return carry

    lax.fori_loop(0, tiles // 2, finish, 0)

    def drain(pair, carry):
        for way in (0, 1):
            for step in range(3):
                hop(2 * pair + way, way, step).wait_send()
        return carry

    lax.fori_loop(0, tiles // 2, drain, 0)
    away_part = o_vm.at[pl.ds(0, blocks - 2)]
    remote(away_part, away_part, o_send, o_recv.at[0], sp, hp).wait_send()


def solution(mesh):
    assert mesh.shape['hp'] == RING and mesh.shape['sp'] == RING * CORES
    ranks = mesh.shape['sp']
    anywhere = pl.BlockSpec(memory_space=pl.ANY)
    dma = pltpu.SemaphoreType.DMA

    def params(ident):
        return pltpu.CompilerParams(collective_id=ident, has_side_effects=True, vmem_limit_bytes=VMEM_BYTES)

    def device_fn(x_loc, w_q, w_k, w_v, w_o):
        rows, depth = x_loc.shape
        width = w_q.shape[1] // ranks
        block = CORES * rows
        blocks = RING * RING
        bf16, f32 = jnp.bfloat16, jnp.float32
        tiles = 16
        cols = w_o.shape[1] // tiles

        qkv = pl.pallas_call(
            qkv_kernel,
            out_shape=jax.ShapeDtypeStruct((3, RING, RING, block, width), bf16),
            in_specs=[anywhere] * 4,
            out_specs=anywhere,
            scratch_shapes=[
                pltpu.VMEM((RING, block, depth), bf16),
                pltpu.VMEM((3, depth, 2 * width), bf16),
                pltpu.VMEM((6 * RING, 2, block, width), bf16),
                pltpu.VMEM((2, 3 * RING, rows, width), bf16),
                dma((5,)), dma((2,)), dma((3, 2)), dma, dma((RING, 2, 2)), dma((3, 2)), dma, dma, dma,
                dma((2, 3 * RING)), dma,
            ],
            compiler_params=params(0),
            name='gather_qkv',
        )(x_loc, w_q, w_k, w_v)

        return pl.pallas_call(
            attend_project_kernel,
            out_shape=jax.ShapeDtypeStruct((rows, w_o.shape[1]), bf16),
            in_specs=[anywhere] * 2,
            out_specs=pl.BlockSpec(memory_space=pltpu.VMEM),
            scratch_shapes=[
                pltpu.VMEM((blocks, block, width), bf16),
                pltpu.VMEM((blocks, block, width), bf16),
                pltpu.VMEM((blocks, width, block), bf16),
                pltpu.VMEM((blocks, block, block), f32),
                pltpu.VMEM((blocks, block, block), f32),
                pltpu.VMEM((min(block, 32), block), f32),
                pltpu.VMEM((min(block, 32), block), f32),
                pltpu.VMEM((blocks, block, width), bf16),
                pltpu.VMEM((RING, ranks, rows, width), bf16),
                pltpu.VMEM((4, w_o.shape[0], cols), bf16),
                pltpu.VMEM((tiles, RING, rows, cols), f32),
                pltpu.VMEM((tiles, 3, rows, cols), f32),
                dma((3,)), dma, dma((RING,)), dma((4,)), dma((tiles, 3)), dma((tiles, 3)),
            ],
            compiler_params=params(1),
            name='attend_project',
        )(qkv.reshape(3, blocks, block, width), w_o)

    seq_spec = P(('dp', 'sp', 'hp'), None)
    in_specs = (seq_spec, P(None, 'hp'), P(None, 'hp'), P(None, 'hp'), P('hp', None))
    return jax.shard_map(device_fn, mesh=mesh, in_specs=in_specs, out_specs=seq_spec, check_vma=False)
```

```python
import functools
import math

import jax
import jax.numpy as jnp
from jax import lax
from jax.experimental import pallas as pl
from jax.experimental.pallas import tpu as pltpu
from jax.sharding import PartitionSpec as P

HEAD_DIM = 128
CORES = 2
RING = 4
MESH_ID = pl.DeviceIdType.MESH
VMEM_BYTES = 66_000_000


def remote(src, dst, send_sem, recv_sem, sp, hp):
    return pltpu.make_async_remote_copy(
        src_ref=src, dst_ref=dst, send_sem=send_sem, recv_sem=recv_sem,
        device_id={'sp': sp, 'hp': hp}, device_id_type=MESH_ID)


def entry_barrier(peers):
    barrier = pltpu.get_barrier_semaphore()
    for sp, hp in peers:
        pl.semaphore_signal(barrier, inc=1, device_id={'sp': sp, 'hp': hp}, device_id_type=MESH_ID)
    pl.semaphore_wait(barrier, len(peers))


def qkv_kernel(x_ref, wq_ref, wk_ref, wv_ref, out_ref, xbuf, wbuf, acc_vm, obuf, via,
               own_send, relay_send, pair_send, load_sem, x_recv, w_sem, out_send, out_recv, out_local, via_recv, via_send):
    sp, hp = lax.axis_index('sp'), lax.axis_index('hp')
    core, chip = lax.rem(sp, CORES), sp // CORES
    partner = sp + 1 - 2 * core
    up, down = lax.rem(hp + 1, RING), lax.rem(hp + RING - 1, RING)
    rows, depth = x_ref.shape
    half, deep = rows // 2, depth // 2
    units, width = wbuf.shape[0], wbuf.shape[2] // 2
    mine, other = core * rows, (1 - core) * rows
    chips = [lax.rem(chip + d, RING) for d in range(RING)]
    ranks = [c * CORES + core for c in chips]
    weights = (wv_ref, wk_ref, wq_ref)
    last = 2 * (RING - 1) * 3

    def slot(p, base, side):
        at = pl.ds(pl.multiple_of(base + side * half, half), half)
        if p < 3:
            return xbuf.at[p, at]
        return xbuf.at[3, at, pl.ds((p - 3) * deep, deep)]

    def unit_copies(u, m, pair, part):
        buf = lax.rem(u, units)
        for n in range(2):
            rank = lax.rem(chip + (2 - pair if n == 0 else 3 * pair), RING) * CORES + core
            yield pltpu.make_async_copy(
                weights[m].at[pl.ds(part * deep, deep), pl.ds(pl.multiple_of(rank * width, width), width)],
                wbuf.at[buf, :, pl.ds(n * width, width)], w_sem.at[buf, n])

    def start_units(step, m, pair):
        for part in range(2):
            for copy in unit_copies(2 * step + part, m, pair, part):
                copy.start()

    def start_far_unit(u, m, pair, part):
        for copy in unit_copies(u, m, pair, part):
            copy.start()

    def wait_unit(u):
        for copy in unit_copies(u, 0, 0, 0):
            copy.wait()

    start_units(jnp.int32(0), 0, 0)
    start_units(jnp.int32(1), 1, 0)
    own_load = pltpu.make_async_copy(x_ref, xbuf.at[0, pl.ds(pl.multiple_of(mine, rows), rows)], load_sem)
    own_load.start()

    entry_barrier([(partner, hp), (sp, up), (sp, down)] + [(ranks[d], hp) for d in (1, 2, 3)])

    first, second = x_ref.at[pl.ds(0, half)], x_ref.at[pl.ds(half, half)]
    own_copies = [
        remote(first, slot(1, mine, 0), own_send.at[1], x_recv.at[1, 0, 0], sp, up),
        remote(second, slot(1, mine, 1), own_send.at[2], x_recv.at[1, 0, 1], sp, down),
        remote(x_ref, xbuf.at[0, pl.ds(pl.multiple_of(mine, rows), rows)], own_send.at[0], x_recv.at[0, 1, 0], partner, hp),
        remote(second, slot(2, mine, 0), own_send.at[3], x_recv.at[2, 0, 0], sp, up),
        remote(first, slot(2, mine, 1), own_send.at[4], x_recv.at[2, 0, 1], sp, down),
    ]
    for copy in own_copies:
        copy.start()

    def arrived(p, k, side):
        place = slot(p, mine if k == 0 else other, side)
        return remote(place, place, own_send.at[0], x_recv.at[p, k, side], sp, hp)

    def to_partner(p, side):
        return remote(slot(p, mine, side), slot(p, mine, side), pair_send.at[p - 1, side], x_recv.at[p, 1, side],
                      partner, hp)

    def relay(part, side):
        at = pl.ds(pl.multiple_of(mine + side * half, half), half)
        return remote(xbuf.at[1, at, pl.ds(part * deep, deep)], slot(3 + part, mine, side), relay_send.at[part, side],
                      x_recv.at[3 + part, 0, side], sp, (up, down)[side])

    def begin_pass(p):
        if p == 0:
            own_load.wait()
            whole = xbuf.at[0, pl.ds(pl.multiple_of(other, rows), rows)]
            remote(whole, whole, own_send.at[0], x_recv.at[0, 1, 0], sp, hp).wait_recv()
            return
        for side in (0, 1):
            arrived(p, 0, side).wait_recv()
            if p == 1:
                for part in range(2):
                    relay(part, side).start()
            to_partner(p, side).start()
        for side in (0, 1):
            arrived(p, 1, side).wait_recv()

    def send_out(g, m):
        p, matrix = g // 2, 2 - m

        @pl.when(lax.rem(g, 2) == 0)
        def _():
            for way in (0, 1):
                remote(obuf.at[g, m, 0, pl.ds(way * rows, rows)], via.at[way, 3 * p + m], out_send,
                       via_recv.at[way, 3 * p + m], ranks[1 + 2 * way], hp).start()
            pltpu.make_async_copy(obuf.at[g, m, 1], out_ref.at[matrix, chip, p], out_local).start()

        @pl.when(lax.rem(g, 2) == 1)
        def _():
            for n, d in enumerate((1, 3)):
                remote(obuf.at[g, m, n], out_ref.at[matrix, chip, p], out_send, out_recv, ranks[d], hp).start()

    def forward(p, m):
        for way in (0, 1):
            spot = via.at[way, 3 * p + m]
            remote(spot, spot, via_send, via_recv.at[way, 3 * p + m], sp, hp).wait_recv()
            remote(spot, out_ref.at[2 - m, chips[3 - 2 * way], p, pl.ds(way * rows, rows)], via_send, out_recv,
                   ranks[1 + 2 * way], hp).start()

    def keep(g, m, prod):
        for n in range(2):
            blk = prod[:, n * width:(n + 1) * width]
            if m == 0:
                blk = blk.T
            obuf[g, m, n] = blk.astype(jnp.bfloat16)

    def settle(g, m):
        if m:
            send_out(g, m - 1)

            @pl.when(lax.rem(g, 2) == 1)
            def _():
                forward(g // 2, m - 1)
        else:
            @pl.when(g > 0)
            def _():
                send_out(g - 1, 2)

            @pl.when((g > 0) & (lax.rem(g, 2) == 0))
            def _():
                forward(g // 2 - 1, 2)

    def full_steps(g, carry):
        p, pair = g // 2, lax.rem(g, 2)
        for m in range(3):
            step = 3 * g + m
            far = step + 2 - last
            ahead, ahead_m = (step + 2) // 3, (m + 2) % 3

            @pl.when(far < 0)
            def _():
                start_units(step + 2, ahead_m, lax.rem(ahead, 2))
            if m:
                @pl.when(far >= 0)
                def _():
                    for n in range(2):
                        start_far_unit(2 * last + 2 * (m - 1) + n, (2 * (m - 1) + n) % 3, (2 * (m - 1) + n) // 3, 0)
            if m == 0:
                for q in range(3):
                    @pl.when(g == 2 * q)
                    def _():
                        begin_pass(q)
            wait_unit(2 * step)
            wait_unit(2 * step + 1)
            buf = lax.rem(2 * step, units)
            prod = (jnp.dot(xbuf[p, :, :deep], wbuf[buf], preferred_element_type=jnp.float32)
                    + jnp.dot(xbuf[p, :, deep:], wbuf[buf + 1], preferred_element_type=jnp.float32))
            keep(g, m, prod)
            settle(g, m)
        return carry

    lax.fori_loop(0, 2 * (RING - 1), full_steps, 0)

    for part in range(2):
        def far_steps(pair, carry):
            g = 2 * (RING - 1) + pair
            for m in range(3):
                t = 6 * part + 3 * pair + m
                nxt = t + 4
                nxt_m = (m + 1) % 3

                @pl.when(nxt < 12)
                def _():
                    if part == 0:
                        within = lax.rem(nxt, 6)
                        for h in range(2):
                            @pl.when(nxt // 6 == h)
                            def _():
                                start_far_unit(2 * last + nxt, nxt_m, within // 3, h)
                    else:
                        start_far_unit(2 * last + nxt, nxt_m, lax.rem(nxt, 6) // 3, 1)
                if m == 0:
                    @pl.when(pair == 0)
                    def _():
                        begin_pass(3 + part)
                u = 2 * last + t
                wait_unit(u)
                prod = jnp.dot(xbuf[3, :, part * deep:(part + 1) * deep], wbuf[lax.rem(u, units)],
                               preferred_element_type=jnp.float32)
                if part == 0:
                    acc_vm[pair, m] = prod
                    if m == 0:
                        @pl.when(pair == 0)
                        def _():
                            send_out(2 * (RING - 1) - 1, 2)
                            forward(RING - 2, 2)
                else:
                    keep(g, m, acc_vm[pair, m] + prod)
                    if m:
                        settle(g, m)
                    else:
                        @pl.when(pair == 1)
                        def _():
                            send_out(g - 1, 2)
            return carry

        lax.fori_loop(0, 2, far_steps, 0)

    for copy in own_copies:
        copy.wait_send()
    send_out(jnp.int32(2 * RING - 1), 2)
    forward(RING - 1, 2)
    for part in range(2):
        for side in (0, 1):
            relay(part, side).wait_send()
    for p in (1, 2, 3, 4):
        for side in (0, 1):
            to_partner(p, side).wait_send()
    local_part = obuf.at[pl.ds(0, RING // 2), :, :]
    pltpu.make_async_copy(local_part, local_part, out_local).wait()
    remote_part = obuf.at[pl.ds(0, 3 * RING // 2), :, :]
    remote(remote_part, remote_part, out_send, out_recv, sp, hp).wait()
    remote(via, via, via_send, out_recv, sp, hp).wait_send()


def attend_project_kernel(qkv_ref, w_ref, y_ref, q_vm, k_vm, vt_vm, s_even, s_odd, m_even, m_odd, o_vm, o_rx, wbuf, part,
                          recv, load_sem, o_send, o_recv, w_sem, send_sem, recv_sem):
    sp, hp = lax.axis_index('sp'), lax.axis_index('hp')
    core, chip = lax.rem(sp, CORES), sp // CORES
    ring = (lax.rem(hp + 1, RING), lax.rem(hp + RING - 1, RING))
    blocks, block = q_vm.shape[0], q_vm.shape[1]
    rows, half = block // 2, block // 4
    ranks, width = o_rx.shape[1], o_rx.shape[3]
    tiles, cols = part.shape[0], part.shape[3]
    lag = blocks // RING
    per_block = tiles // (2 * lag)
    depth = wbuf.shape[0]
    scale = HEAD_DIM ** -0.5 * math.log2(math.e)
    strip = min(block, 32)

    loads = [pltpu.make_async_copy(qkv_ref.at[m], dst, load_sem.at[m]) for m, dst in enumerate((q_vm, k_vm, vt_vm))]
    for copy in loads:
        copy.start()

    def w_copy(n):
        tile, buf = lax.rem(n, tiles), lax.rem(n, depth)
        return pltpu.make_async_copy(w_ref.at[:, pl.ds(pl.multiple_of(tile * cols, cols), cols)], wbuf.at[buf],
                                     w_sem.at[buf])

    for n in range(depth - 1):
        w_copy(jnp.int32(n)).start()
    others = [(d, k) for d in range(RING) for k in range(CORES) if (d, k) != (0, 0)]
    rank_of = lambda d, k: lax.rem(chip + d, RING) * CORES + lax.rem(core + k, CORES)
    entry_barrier([(rank_of(d, k), hp) for d, k in others] + [(sp, ring[0]), (sp, ring[1])])
    for copy in loads:
        copy.wait()

    def which(i):
        return lax.rem(chip + 1 + lax.rem(i, RING), RING) * RING + lax.rem(i // RING + 1, RING)

    def lanes(head):
        return slice(head * HEAD_DIM, (head + 1) * HEAD_DIM)

    def scores(q_blk, head, chunk):
        return lax.dot_general(k_vm[chunk, :, lanes(head)], q_blk, (((1,), (1,)), ((), ())),
                               preferred_element_type=jnp.float32)

    def fold(x, op):
        parts = x.reshape(block // strip, strip, block)
        return op(parts, axis=0)

    def stage(q_next, next_head, s_next, m_next, s_now, m_now, head):
        shift = None if s_now is None else jnp.max(m_now[...], axis=0, keepdims=True) * scale
        peak = total = acc = None
        for chunk in range(blocks):
            s = scores(q_next, next_head, chunk)
            s_next[chunk] = s
            top = fold(s, jnp.max)
            peak = top if peak is None else jnp.maximum(peak, top)
            if s_now is not None:
                prob = jnp.exp2(s_now[chunk] * scale - shift)
                add = fold(prob, jnp.sum)
                total = add if total is None else total + add
                pv = jnp.dot(vt_vm[chunk, lanes(head), :], prob.astype(jnp.bfloat16), preferred_element_type=jnp.float32)
                acc = pv if acc is None else acc + pv
        m_next[...] = peak
        if s_now is None:
            return None
        return (acc / jnp.sum(total, axis=0, keepdims=True)).T.astype(jnp.bfloat16)

    stage(q_vm[which(0), :, lanes(0)], 0, s_even, m_even, None, None, 0)

    def send_home(i):
        d, turn_no = lax.rem(i + 1, RING), i // RING
        home = lax.rem(chip + d, RING) * CORES
        for k in range(CORES):
            kk = lax.rem(core + k, CORES)
            piece = pl.ds(pl.multiple_of(kk * rows, rows), rows)

            def away():
                remote(o_vm.at[i, piece], o_rx.at[turn_no, sp], o_send, o_recv.at[turn_no], home + kk, hp).start()

            if k:
                away()
            else:
                pl.when(d != 0)(away)

                @pl.when(d == 0)
                def _():
                    o_rx[turn_no, sp] = o_vm[i, piece]

    order = ((1, 3, 2), (2, 3, 1))

    def hop(tile, way, step):
        return remote(part.at[tile, order[way][step]], recv.at[tile, step], send_sem.at[tile, step],
                      recv_sem.at[tile, step], sp, ring[way])

    def spot(turn_no, side):
        late, second = turn_no // 2, lax.rem(turn_no, 2)
        slot = (1 - late) * (1 + side) + late * (3 - 3 * second)
        first = (1 - late) * second * (1 - 2 * side) + side
        return slot, pl.ds(pl.multiple_of(first * half, half), half)

    def ship(n, way):
        turn_no, tile = n // tiles, lax.rem(n, tiles)

        @pl.when(turn_no < 2)
        def _():
            _, piece = spot(turn_no, way)
            remote(part.at[tile, order[way][0], piece], recv.at[tile, 0, piece], send_sem.at[tile, 0],
                   recv_sem.at[tile, 0], sp, ring[way]).start()

        @pl.when(turn_no == 2)
        def _():
            hop(tile, way, 1).start()

    def project(pair):
        turn_no = pair // (tiles // 2)

        @pl.when(lax.rem(pair, tiles // 2) == 0)
        def _():
            seven = o_rx.at[turn_no, pl.ds(0, ranks - 1)]
            remote(seven, seven, o_send, o_recv.at[turn_no], sp, hp).wait_recv()

        for way in (0, 1):
            n = 2 * pair + way
            tile, buf = lax.rem(n, tiles), lax.rem(n, depth)

            @pl.when(n + depth - 1 < RING * tiles)
            def _():
                w_copy(n + depth - 1).start()
            w_copy(n).wait()
            acc = None
            for r in range(ranks):
                prod = jnp.dot(o_rx[turn_no, r], wbuf[buf, pl.ds(r * width, width), :],
                               preferred_element_type=jnp.float32)
                acc = prod if acc is None else acc + prod
            for side in (0, 1):
                slot, piece = spot(turn_no, side)
                part[tile, slot, piece] = acc[side * half:(side + 1) * half]

            @pl.when(turn_no == 2)
            def _():
                hop(tile, way, 0).wait_recv()
                part[tile, 3] = part[tile, 3] + recv[tile, 0]

            @pl.when(n > 0)
            def _():
                ship(n - 1, 1 - way)

    def body(i, carry):
        @pl.when(i > 0)
        def _():
            send_home(i - 1)
        now, later = which(i), which(lax.rem(i + 1, blocks))
        o_vm[i, :, lanes(0)] = stage(q_vm[now, :, lanes(1)], 1, s_odd, m_odd, s_even, m_even, 0)

        @pl.when(i >= lag)
        def _():
            project(per_block * (i - lag))
        o_vm[i, :, lanes(1)] = stage(q_vm[later, :, lanes(0)], 0, s_even, m_even, s_odd, m_odd, 1)

        @pl.when(i >= lag)
        def _():
            project(per_block * (i - lag) + 1)
        return carry

    lax.fori_loop(0, blocks, body, 0)
    send_home(jnp.int32(blocks - 1))

    def last_round(pair, carry):
        project(pair)
        return carry

    lax.fori_loop(per_block * (blocks - lag), per_block * blocks, last_round, 0)

    def pass_on(pair, carry):
        for way in (0, 1):
            tile = 2 * pair + way
            hop(tile, way, 1).wait_recv()
            slot = order[way][2]
            part[tile, slot] = part[tile, slot] + recv[tile, 1]
        for way in (0, 1):
            hop(2 * pair + way, way, 2).start()
        return carry

    lax.fori_loop(0, tiles // 2, pass_on, 0)

    def finish(pair, carry):
        for way in (0, 1):
            tile = 2 * pair + way
            hop(tile, way, 2).wait_recv()
            y_ref[:, pl.ds(pl.multiple_of(tile * cols, cols), cols)] = (part[tile, 0] + recv[tile, 2]).astype(y_ref.dtype)
        return carry

    lax.fori_loop(0, tiles // 2, finish, 0)

    def drain(pair, carry):
        for way in (0, 1):
            for step in range(3):
                hop(2 * pair + way, way, step).wait_send()
        return carry

    lax.fori_loop(0, tiles // 2, drain, 0)
    away_part = o_vm.at[pl.ds(0, blocks - 2)]
    remote(away_part, away_part, o_send, o_recv.at[0], sp, hp).wait_send()


def solution(mesh):
    assert mesh.shape['hp'] == RING and mesh.shape['sp'] == RING * CORES
    ranks = mesh.shape['sp']
    anywhere = pl.BlockSpec(memory_space=pl.ANY)
    dma = pltpu.SemaphoreType.DMA

    def params(ident):
        return pltpu.CompilerParams(collective_id=ident, has_side_effects=True, vmem_limit_bytes=VMEM_BYTES)

    def device_fn(x_loc, w_q, w_k, w_v, w_o):
        rows, depth = x_loc.shape
        width = w_q.shape[1] // ranks
        block = CORES * rows
        assert block == width
        blocks = RING * RING
        bf16, f32 = jnp.bfloat16, jnp.float32
        tiles = 16
        cols = w_o.shape[1] // tiles

        qkv = pl.pallas_call(
            qkv_kernel,
            out_shape=jax.ShapeDtypeStruct((3, RING, RING, block, width), bf16),
            in_specs=[anywhere] * 4,
            out_specs=anywhere,
            scratch_shapes=[
                pltpu.VMEM((RING, block, depth), bf16),
                pltpu.VMEM((6, depth // 2, 2 * width), bf16),
                pltpu.VMEM((2, 3, block, 2 * width), f32),
                pltpu.VMEM((2 * RING, 3, 2, block, width), bf16),
                pltpu.VMEM((2, 3 * RING, rows, width), bf16),
                dma((5,)), dma((2, 2)), dma((4, 2)), dma, dma((RING + 1, 2, 2)), dma((6, 2)), dma, dma, dma,
                dma((2, 3 * RING)), dma,
            ],
            compiler_params=params(0),
            name='gather_qkv',
        )(x_loc, w_q, w_k, w_v)

        return pl.pallas_call(
            attend_project_kernel,
            out_shape=jax.ShapeDtypeStruct((rows, w_o.shape[1]), bf16),
            in_specs=[anywhere] * 2,
            out_specs=pl.BlockSpec(memory_space=pltpu.VMEM),
            scratch_shapes=[
                pltpu.VMEM((blocks, block, width), bf16),
                pltpu.VMEM((blocks, block, width), bf16),
                pltpu.VMEM((blocks, width, block), bf16),
                pltpu.VMEM((blocks, block, block), f32),
                pltpu.VMEM((blocks, block, block), f32),
                pltpu.VMEM((min(block, 32), block), f32),
                pltpu.VMEM((min(block, 32), block), f32),
                pltpu.VMEM((blocks, block, width), bf16),
                pltpu.VMEM((RING, ranks, rows, width), bf16),
                pltpu.VMEM((4, w_o.shape[0], cols), bf16),
                pltpu.VMEM((tiles, RING, rows, cols), f32),
                pltpu.VMEM((tiles, 3, rows, cols), f32),
                dma((3,)), dma, dma((RING,)), dma((4,)), dma((tiles, 3)), dma((tiles, 3)),
            ],
            compiler_params=params(1),
            name='attend_project',
        )(qkv.reshape(3, blocks, block, width), w_o)

    seq_spec = P(('dp', 'sp', 'hp'), None)
    in_specs = (seq_spec, P(None, 'hp'), P(None, 'hp'), P(None, 'hp'), P('hp', None))
    return jax.shard_map(device_fn, mesh=mesh, in_specs=in_specs, out_specs=seq_spec, check_vma=False)
```

```python
import functools
import math

import jax
import jax.numpy as jnp
from jax import lax
from jax.experimental import pallas as pl
from jax.experimental.pallas import tpu as pltpu
from jax.sharding import PartitionSpec as P

HEAD_DIM = 128
CORES = 2
RING = 4
MESH_ID = pl.DeviceIdType.MESH
VMEM_BYTES = 66_000_000


def remote(src, dst, send_sem, recv_sem, sp, hp):
    return pltpu.make_async_remote_copy(
        src_ref=src, dst_ref=dst, send_sem=send_sem, recv_sem=recv_sem,
        device_id={'sp': sp, 'hp': hp}, device_id_type=MESH_ID)


def entry_barrier(peers):
    barrier = pltpu.get_barrier_semaphore()
    for sp, hp in peers:
        pl.semaphore_signal(barrier, inc=1, device_id={'sp': sp, 'hp': hp}, device_id_type=MESH_ID)
    pl.semaphore_wait(barrier, len(peers))


def qkv_kernel(x_ref, wq_ref, wk_ref, wv_ref, out_ref, xbuf, wbuf, acc_vm, obuf, via,
               own_send, relay_send, pair_send, load_sem, x_recv, w_sem, out_send, out_recv, out_local, via_recv, via_send):
    sp, hp = lax.axis_index('sp'), lax.axis_index('hp')
    core, chip = lax.rem(sp, CORES), sp // CORES
    partner = sp + 1 - 2 * core
    up, down = lax.rem(hp + 1, RING), lax.rem(hp + RING - 1, RING)
    rows, depth = x_ref.shape
    half, deep = rows // 2, depth // 2
    units, width = wbuf.shape[0], wbuf.shape[2] // 2
    mine, other = core * rows, (1 - core) * rows
    chips = [lax.rem(chip + d, RING) for d in range(RING)]
    ranks = [c * CORES + core for c in chips]
    weights = (wv_ref, wk_ref, wq_ref)
    last = 2 * (RING - 1) * 3

    def slot(p, base, side):
        at = pl.ds(pl.multiple_of(base + side * half, half), half)
        if p < 3:
            return xbuf.at[p, at]
        return xbuf.at[3, at, pl.ds((p - 3) * deep, deep)]

    def unit_copies(u, m, pair, part):
        buf = lax.rem(u, units)
        for n in range(2):
            rank = lax.rem(chip + (2 - pair if n == 0 else 3 * pair), RING) * CORES + core
            yield pltpu.make_async_copy(
                weights[m].at[pl.ds(part * deep, deep), pl.ds(pl.multiple_of(rank * width, width), width)],
                wbuf.at[buf, :, pl.ds(n * width, width)], w_sem.at[buf, n])

    def start_units(step, m, pair):
        for part in range(2):
            for copy in unit_copies(2 * step + part, m, pair, part):
                copy.start()

    def start_far_unit(u, m, pair, part):
        for copy in unit_copies(u, m, pair, part):
            copy.start()

    def wait_unit(u):
        for copy in unit_copies(u, 0, 0, 0):
            copy.wait()

    start_units(jnp.int32(0), 0, 0)
    start_units(jnp.int32(1), 1, 0)
    own_load = pltpu.make_async_copy(x_ref, xbuf.at[0, pl.ds(pl.multiple_of(mine, rows), rows)], load_sem)
    own_load.start()

    entry_barrier([(partner, hp), (sp, up), (sp, down)] + [(ranks[d], hp) for d in (1, 2, 3)])

    first, second = x_ref.at[pl.ds(0, half)], x_ref.at[pl.ds(half, half)]
    own_copies = [
        remote(first, slot(1, mine, 0), own_send.at[1], x_recv.at[1, 0, 0], sp, up),
        remote(second, slot(1, mine, 1), own_send.at[2], x_recv.at[1, 0, 1], sp, down),
        remote(x_ref, xbuf.at[0, pl.ds(pl.multiple_of(mine, rows), rows)], own_send.at[0], x_recv.at[0, 1, 0], partner, hp),
        remote(second, slot(2, mine, 0), own_send.at[3], x_recv.at[2, 0, 0], sp, up),
        remote(first, slot(2, mine, 1), own_send.at[4], x_recv.at[2, 0, 1], sp, down),
    ]
    for copy in own_copies:
        copy.start()

    def arrived(p, k, side):
        place = slot(p, mine if k == 0 else other, side)
        return remote(place, place, own_send.at[0], x_recv.at[p, k, side], sp, hp)

    def to_partner(p, side):
        return remote(slot(p, mine, side), slot(p, mine, side), pair_send.at[p - 1, side], x_recv.at[p, 1, side],
                      partner, hp)

    def relay(part, side):
        at = pl.ds(pl.multiple_of(mine + side * half, half), half)
        return remote(xbuf.at[1, at, pl.ds(part * deep, deep)], slot(3 + part, mine, side), relay_send.at[part, side],
                      x_recv.at[3 + part, 0, side], sp, (up, down)[side])

    def begin_pass(p):
        if p == 0:
            own_load.wait()
            whole = xbuf.at[0, pl.ds(pl.multiple_of(other, rows), rows)]
            remote(whole, whole, own_send.at[0], x_recv.at[0, 1, 0], sp, hp).wait_recv()
            return
        for side in (0, 1):
            arrived(p, 0, side).wait_recv()
            if p == 1:
                for part in range(2):
                    relay(part, side).start()
            to_partner(p, side).start()
        for side in (0, 1):
            arrived(p, 1, side).wait_recv()

    def send_out(g, m):
        p, matrix = g // 2, 2 - m

        @pl.when(lax.rem(g, 2) == 0)
        def _():
            for way in (0, 1):
                remote(obuf.at[g, m, 0, pl.ds(way * rows, rows)], via.at[way, 3 * p + m], out_send,
                       via_recv.at[way, 3 * p + m], ranks[1 + 2 * way], hp).start()
            pltpu.make_async_copy(obuf.at[g, m, 1], out_ref.at[matrix, chip, p], out_local).start()

        @pl.when(lax.rem(g, 2) == 1)
        def _():
            for n, d in enumerate((1, 3)):
                remote(obuf.at[g, m, n], out_ref.at[matrix, chip, p], out_send, out_recv, ranks[d], hp).start()

    def forward(p, m):
        for way in (0, 1):
            spot = via.at[way, 3 * p + m]
            remote(spot, spot, via_send, via_recv.at[way, 3 * p + m], sp, hp).wait_recv()
            remote(spot, out_ref.at[2 - m, chips[3 - 2 * way], p, pl.ds(way * rows, rows)], via_send, out_recv,
                   ranks[1 + 2 * way], hp).start()

    def keep(g, m, prod):
        for n in range(2):
            blk = prod[:, n * width:(n + 1) * width]
            if m == 0:
                blk = blk.T
            obuf[g, m, n] = blk.astype(jnp.bfloat16)

    def settle(g, m):
        if m:
            send_out(g, m - 1)

            @pl.when(lax.rem(g, 2) == 1)
            def _():
                forward(g // 2, m - 1)
        else:
            @pl.when(g > 0)
            def _():
                send_out(g - 1, 2)

            @pl.when((g > 0) & (lax.rem(g, 2) == 0))
            def _():
                forward(g // 2 - 1, 2)

    def full_steps(g, carry):
        p, pair = g // 2, lax.rem(g, 2)
        for m in range(3):
            step = 3 * g + m
            far = step + 2 - last
            ahead, ahead_m = (step + 2) // 3, (m + 2) % 3

            @pl.when(far < 0)
            def _():
                start_units(step + 2, ahead_m, lax.rem(ahead, 2))
            if m:
                @pl.when(far >= 0)
                def _():
                    for n in range(2):
                        start_far_unit(2 * last + 2 * (m - 1) + n, (2 * (m - 1) + n) % 3, (2 * (m - 1) + n) // 3, 0)
            if m == 0:
                for q in range(3):
                    @pl.when(g == 2 * q)
                    def _():
                        begin_pass(q)
            wait_unit(2 * step)
            wait_unit(2 * step + 1)
            buf = lax.rem(2 * step, units)
            prod = (jnp.dot(xbuf[p, :, :deep], wbuf[buf], preferred_element_type=jnp.float32)
                    + jnp.dot(xbuf[p, :, deep:], wbuf[buf + 1], preferred_element_type=jnp.float32))
            keep(g, m, prod)
            settle(g, m)
        return carry

    lax.fori_loop(0, 2 * (RING - 1), full_steps, 0)

    for part in range(2):
        def far_steps(pair, carry):
            g = 2 * (RING - 1) + pair
            for m in range(3):
                t = 6 * part + 3 * pair + m
                nxt = t + 4
                nxt_m = (m + 1) % 3

                @pl.when(nxt < 12)
                def _():
                    if part == 0:
                        within = lax.rem(nxt, 6)
                        for h in range(2):
                            @pl.when(nxt // 6 == h)
                            def _():
                                start_far_unit(2 * last + nxt, nxt_m, within // 3, h)
                    else:
                        start_far_unit(2 * last + nxt, nxt_m, lax.rem(nxt, 6) // 3, 1)
                if m == 0:
                    @pl.when(pair == 0)
                    def _():
                        begin_pass(3 + part)
                u = 2 * last + t
                wait_unit(u)
                prod = jnp.dot(xbuf[3, :, part * deep:(part + 1) * deep], wbuf[lax.rem(u, units)],
                               preferred_element_type=jnp.float32)
                if part == 0:
                    acc_vm[pair, m] = prod
                    if m == 0:
                        @pl.when(pair == 0)
                        def _():
                            send_out(2 * (RING - 1) - 1, 2)
                            forward(RING - 2, 2)
                else:
                    keep(g, m, acc_vm[pair, m] + prod)
                    if m:
                        settle(g, m)
                    else:
                        @pl.when(pair == 1)
                        def _():
                            send_out(g - 1, 2)
            return carry

        lax.fori_loop(0, 2, far_steps, 0)

    for copy in own_copies:
        copy.wait_send()
    send_out(jnp.int32(2 * RING - 1), 2)
    forward(RING - 1, 2)
    for part in range(2):
        for side in (0, 1):
            relay(part, side).wait_send()
    for p in (1, 2, 3, 4):
        for side in (0, 1):
            to_partner(p, side).wait_send()
    local_part = obuf.at[pl.ds(0, RING // 2), :, :]
    pltpu.make_async_copy(local_part, local_part, out_local).wait()
    remote_part = obuf.at[pl.ds(0, 3 * RING // 2), :, :]
    remote(remote_part, remote_part, out_send, out_recv, sp, hp).wait()
    remote(via, via, via_send, out_recv, sp, hp).wait_send()


def attend_project_kernel(qkv_ref, w_ref, y_ref, q_vm, k_vm, vt_vm, s_even, s_odd, m_even, m_odd, o_vm, o_rx, wbuf, part,
                          recv, load_sem, o_send, o_recv, w_sem, send_sem, recv_sem):
    sp, hp = lax.axis_index('sp'), lax.axis_index('hp')
    core, chip = lax.rem(sp, CORES), sp // CORES
    ring = (lax.rem(hp + 1, RING), lax.rem(hp + RING - 1, RING))
    blocks, block = q_vm.shape[0], q_vm.shape[1]
    rows, half = block // 2, block // 4
    ranks, width = o_rx.shape[1], o_rx.shape[3]
    tiles, cols = part.shape[0], part.shape[3]
    lag = blocks // RING
    per_block = tiles // (2 * lag)
    depth = wbuf.shape[0]
    scale = HEAD_DIM ** -0.5 * math.log2(math.e)
    strip = min(block, 32)

    loads = [pltpu.make_async_copy(qkv_ref.at[m], dst, load_sem.at[m]) for m, dst in enumerate((q_vm, k_vm, vt_vm))]
    for copy in loads:
        copy.start()

    def w_copy(n):
        tile, buf = lax.rem(n, tiles), lax.rem(n, depth)
        return pltpu.make_async_copy(w_ref.at[:, pl.ds(pl.multiple_of(tile * cols, cols), cols)], wbuf.at[buf],
                                     w_sem.at[buf])

    for n in range(depth - 1):
        w_copy(jnp.int32(n)).start()
    others = [(d, k) for d in range(RING) for k in range(CORES) if (d, k) != (0, 0)]
    rank_of = lambda d, k: lax.rem(chip + d, RING) * CORES + lax.rem(core + k, CORES)
    entry_barrier([(rank_of(d, k), hp) for d, k in others] + [(sp, ring[0]), (sp, ring[1])])
    for copy in loads[:2]:
        copy.wait()

    def which(i):
        return lax.rem(chip + 1 + lax.rem(i, RING), RING) * RING + lax.rem(i // RING + 1, RING)

    def lanes(head):
        return slice(head * HEAD_DIM, (head + 1) * HEAD_DIM)

    def scores(q_blk, head, chunk):
        return lax.dot_general(k_vm[chunk, :, lanes(head)], q_blk, (((1,), (1,)), ((), ())),
                               preferred_element_type=jnp.float32)

    def fold(x, op):
        parts = x.reshape(block // strip, strip, block)
        return op(parts, axis=0)

    def stage(q_next, next_head, s_next, m_next, s_now, m_now, head):
        shift = None if s_now is None else jnp.max(m_now[...], axis=0, keepdims=True) * scale
        peak = total = acc = None
        for chunk in range(blocks):
            s = scores(q_next, next_head, chunk)
            s_next[chunk] = s
            top = fold(s, jnp.max)
            peak = top if peak is None else jnp.maximum(peak, top)
            if s_now is not None:
                prob = jnp.exp2(s_now[chunk] * scale - shift)
                add = fold(prob, jnp.sum)
                total = add if total is None else total + add
                pv = jnp.dot(vt_vm[chunk, lanes(head), :], prob.astype(jnp.bfloat16), preferred_element_type=jnp.float32)
                acc = pv if acc is None else acc + pv
        m_next[...] = peak
        if s_now is None:
            return None
        return (acc / jnp.sum(total, axis=0, keepdims=True)).T.astype(jnp.bfloat16)

    stage(q_vm[which(0), :, lanes(0)], 0, s_even, m_even, None, None, 0)
    loads[2].wait()

    def send_home(i):
        d, turn_no = lax.rem(i + 1, RING), i // RING
        home = lax.rem(chip + d, RING) * CORES
        for k in range(CORES):
            kk = lax.rem(core + k, CORES)
            piece = pl.ds(pl.multiple_of(kk * rows, rows), rows)

            def away():
                remote(o_vm.at[i, piece], o_rx.at[turn_no, sp], o_send, o_recv.at[turn_no], home + kk, hp).start()

            if k:
                away()
            else:
                pl.when(d != 0)(away)

                @pl.when(d == 0)
                def _():
                    o_rx[turn_no, sp] = o_vm[i, piece]

    order = ((1, 3, 2), (2, 3, 1))

    def hop(tile, way, step):
        return remote(part.at[tile, order[way][step]], recv.at[tile, step], send_sem.at[tile, step],
                      recv_sem.at[tile, step], sp, ring[way])

    def spot(turn_no, side):
        late, second = turn_no // 2, lax.rem(turn_no, 2)
        slot = (1 - late) * (1 + side) + late * (3 - 3 * second)
        first = (1 - late) * second * (1 - 2 * side) + side
        return slot, pl.ds(pl.multiple_of(first * half, half), half)

    def ship(n, way):
        turn_no, tile = n // tiles, lax.rem(n, tiles)

        @pl.when(turn_no < 2)
        def _():
            _, piece = spot(turn_no, way)
            remote(part.at[tile, order[way][0], piece], recv.at[tile, 0, piece], send_sem.at[tile, 0],
                   recv_sem.at[tile, 0], sp, ring[way]).start()

        @pl.when(turn_no == 2)
        def _():
            hop(tile, way, 1).start()

    def project(pair):
        turn_no = pair // (tiles // 2)

        @pl.when(lax.rem(pair, tiles // 2) == 0)
        def _():
            seven = o_rx.at[turn_no, pl.ds(0, ranks - 1)]
            remote(seven, seven, o_send, o_recv.at[turn_no], sp, hp).wait_recv()

        for way in (0, 1):
            n = 2 * pair + way
            tile, buf = lax.rem(n, tiles), lax.rem(n, depth)

            @pl.when(n + depth - 1 < RING * tiles)
            def _():
                w_copy(n + depth - 1).start()
            w_copy(n).wait()
            acc = None
            for r in range(ranks):
                prod = jnp.dot(o_rx[turn_no, r], wbuf[buf, pl.ds(r * width, width), :],
                               preferred_element_type=jnp.float32)
                acc = prod if acc is None else acc + prod
            for side in (0, 1):
                slot, piece = spot(turn_no, side)
                part[tile, slot, piece] = acc[side * half:(side + 1) * half]

            @pl.when(turn_no == 2)
            def _():
                hop(tile, way, 0).wait_recv()
                part[tile, 3] = part[tile, 3] + recv[tile, 0]
        for way in (0, 1):
            ship(2 * pair + way, way)

    def body(i, carry):
        @pl.when(i > 0)
        def _():
            send_home(i - 1)
        now, later = which(i), which(lax.rem(i + 1, blocks))
        o_vm[i, :, lanes(0)] = stage(q_vm[now, :, lanes(1)], 1, s_odd, m_odd, s_even, m_even, 0)

        @pl.when(i >= lag)
        def _():
            project(per_block * (i - lag))
        o_vm[i, :, lanes(1)] = stage(q_vm[later, :, lanes(0)], 0, s_even, m_even, s_odd, m_odd, 1)

        @pl.when(i >= lag)
        def _():
            project(per_block * (i - lag) + 1)
        return carry

    lax.fori_loop(0, blocks, body, 0)
    send_home(jnp.int32(blocks - 1))

    def last_round(pair, carry):
        project(pair)
        return carry

    lax.fori_loop(per_block * (blocks - lag), per_block * blocks, last_round, 0)

    def pass_on(pair, carry):
        for way in (0, 1):
            tile = 2 * pair + way
            hop(tile, way, 1).wait_recv()
            slot = order[way][2]
            part[tile, slot] = part[tile, slot] + recv[tile, 1]
        for way in (0, 1):
            hop(2 * pair + way, way, 2).start()
        return carry

    lax.fori_loop(0, tiles // 2, pass_on, 0)

    def finish(pair, carry):
        for way in (0, 1):
            tile = 2 * pair + way
            hop(tile, way, 2).wait_recv()
            y_ref[:, pl.ds(pl.multiple_of(tile * cols, cols), cols)] = (part[tile, 0] + recv[tile, 2]).astype(y_ref.dtype)
        return carry

    lax.fori_loop(0, tiles // 2, finish, 0)

    def drain(pair, carry):
        for way in (0, 1):
            for step in range(3):
                hop(2 * pair + way, way, step).wait_send()
        return carry

    lax.fori_loop(0, tiles // 2, drain, 0)
    away_part = o_vm.at[pl.ds(0, blocks - 2)]
    remote(away_part, away_part, o_send, o_recv.at[0], sp, hp).wait_send()


def solution(mesh):
    assert mesh.shape['hp'] == RING and mesh.shape['sp'] == RING * CORES
    ranks = mesh.shape['sp']
    anywhere = pl.BlockSpec(memory_space=pl.ANY)
    dma = pltpu.SemaphoreType.DMA

    def params(ident):
        return pltpu.CompilerParams(collective_id=ident, has_side_effects=True, vmem_limit_bytes=VMEM_BYTES)

    def device_fn(x_loc, w_q, w_k, w_v, w_o):
        rows, depth = x_loc.shape
        width = w_q.shape[1] // ranks
        block = CORES * rows
        assert block == width
        blocks = RING * RING
        bf16, f32 = jnp.bfloat16, jnp.float32
        tiles = 16
        cols = w_o.shape[1] // tiles

        qkv = pl.pallas_call(
            qkv_kernel,
            out_shape=jax.ShapeDtypeStruct((3, RING, RING, block, width), bf16),
            in_specs=[anywhere] * 4,
            out_specs=anywhere,
            scratch_shapes=[
                pltpu.VMEM((RING, block, depth), bf16),
                pltpu.VMEM((6, depth // 2, 2 * width), bf16),
                pltpu.VMEM((2, 3, block, 2 * width), f32),
                pltpu.VMEM((2 * RING, 3, 2, block, width), bf16),
                pltpu.VMEM((2, 3 * RING, rows, width), bf16),
                dma((5,)), dma((2, 2)), dma((4, 2)), dma, dma((RING + 1, 2, 2)), dma((6, 2)), dma, dma, dma,
                dma((2, 3 * RING)), dma,
            ],
            compiler_params=params(0),
            name='gather_qkv',
        )(x_loc, w_q, w_k, w_v)

        return pl.pallas_call(
            attend_project_kernel,
            out_shape=jax.ShapeDtypeStruct((rows, w_o.shape[1]), bf16),
            in_specs=[anywhere] * 2,
            out_specs=pl.BlockSpec(memory_space=pltpu.VMEM),
            scratch_shapes=[
                pltpu.VMEM((blocks, block, width), bf16),
                pltpu.VMEM((blocks, block, width), bf16),
                pltpu.VMEM((blocks, width, block), bf16),
                pltpu.VMEM((blocks, block, block), f32),
                pltpu.VMEM((blocks, block, block), f32),
                pltpu.VMEM((min(block, 32), block), f32),
                pltpu.VMEM((min(block, 32), block), f32),
                pltpu.VMEM((blocks, block, width), bf16),
                pltpu.VMEM((RING, ranks, rows, width), bf16),
                pltpu.VMEM((4, w_o.shape[0], cols), bf16),
                pltpu.VMEM((tiles, RING, rows, cols), f32),
                pltpu.VMEM((tiles, 3, rows, cols), f32),
                dma((3,)), dma, dma((RING,)), dma((4,)), dma((tiles, 3)), dma((tiles, 3)),
            ],
            compiler_params=params(1),
            name='attend_project',
        )(qkv.reshape(3, blocks, block, width), w_o)

    seq_spec = P(('dp', 'sp', 'hp'), None)
    in_specs = (seq_spec, P(None, 'hp'), P(None, 'hp'), P(None, 'hp'), P('hp', None))
    return jax.shard_map(device_fn, mesh=mesh, in_specs=in_specs, out_specs=seq_spec, check_vma=False)
```
